128 devices in a mesh: section: 4 (over x), dp: 32 (over y, z, core).
Axes of the slice: x: 4, y: 4, z: 4, core: 2. Of those that a mesh axis runs over, the one named last changes fastest.
Arguments:
- clip_pool: bfloat16 [1024, 256, 512], P('dp'), may hold values from -8 to 8
- clip_index: int32 [8, 128], P(None, 'dp'), may hold values from 0 to 31, as said below
- batch_order: int32 [8], replicated, may hold values from 0 to 7, each once
- tap_weights: bfloat16 [4, 3, 512, 512], P('section'), may hold values from -0.15625 to 0.15625
- out_weights: bfloat16 [4, 512, 512], P('section'), may hold values from -0.25 to 0.25
- norm_gains: bfloat16 [4, 512], P('section'), may hold values from 0.099609375 to 1.8984375
- quant_weight: bfloat16 [512, 18], replicated, may hold values from -0.25 to 0.25
- quant_bias: float32 [18], replicated, may hold values from -3 to 3
- post_weight: bfloat16 [18, 512], replicated, may hold values from -1.5 to 1.5
Outputs:
- row_error: float32 [8, 128, 256], P('section', 'dp')
- entropy_loss: float32 [8], replicated
The draws below stay inside these ranges and needn't reach their ends.
Inputs may be any that keep to these rules, and one draw needn't show every extreme that they name: `clip_index`: entries index the clips of the replica that holds the column; over all 8 micro-batches, the 4 columns of one replica name each of its 32 clips exactly once. `batch_order`: each micro-batch number 0 to 7 once.
All inputs are finite; a program needn't handle non-finite values.
Results may differ from the reference program's by a relative error of at most 0.0015.
Values may be sent and summed in bfloat16 or wider, within the bound.
A program may use at most 128 MiB of HBM per device.

```python
import jax
import jax.numpy as jnp
from jax import lax

C = 512
BITS = 18
TAPS = 3
SPATIAL = 64
CLIPS = 4
MB = 8
POOL = 32
ROWS = 256
CL_ALL = 128
POOL_ALL = 1024
N_SECTION = 4


def draw_clip_pool(key, part):
    first, second, third = jax.random.split(jax.random.fold_in(key, 17), 3)
    offset = jax.random.normal(first, (POOL_ALL, 1, C), jnp.float32)
    noise = jax.random.normal(second, (POOL_ALL, ROWS, C), jnp.float32)
    value = jnp.clip(0.8 * offset + 0.6 * noise, -8.0, 8.0)
    return value.astype(jnp.bfloat16)


def draw_clip_index(key, part):
    groups = CL_ALL // CLIPS
    keys = jax.random.split(jax.random.fold_in(key, 29), groups)
    ordered = jnp.arange(POOL, dtype=jnp.int32)
    shuffled = jax.vmap(lambda single: jax.random.permutation(single, ordered))(keys)
    arranged = shuffled.reshape(groups, MB, CLIPS).transpose(1, 0, 2)
    return arranged.reshape(MB, CL_ALL).astype(jnp.int32)


def levels(stream_key, shape, pieces, least, high):
    level, own = 1.0, jax.random.fold_in(stream_key, 6)
    for dim, parts in pieces:
        draws = jnp.exp(jax.random.uniform(jax.random.fold_in(own, dim), (parts,), jnp.float32, least / len(pieces), high / len(pieces)))
        level = level * jnp.repeat(draws, shape[dim] // parts).reshape([-1 if axis == dim else 1 for axis in range(len(shape))])
    return level


def normal_values(key, extent, deviation, reach, shards=(), kind=jnp.bfloat16):
    drawn = deviation * jax.random.normal(key, extent, jnp.float32)
    if shards:
        drawn = drawn * levels(key, extent, shards, -0.22, 0.18)
    return jnp.clip(drawn, -reach, reach).astype(kind)


def setup_inputs(seed: int = 0) -> dict:
    splits = jax.random.split(jax.random.key(seed), 10)
    return {
        "clip_pool": draw_clip_pool(jax.random.fold_in(splits[9], 71), 0),
        "clip_index": draw_clip_index(jax.random.fold_in(splits[9], 71), 0),
        "batch_order": jax.random.permutation(splits[2], MB).astype(jnp.int32),
        "tap_weights": normal_values(splits[3], (N_SECTION, TAPS, C, C), (TAPS * C) ** -0.5, 0.15625, ((0, 4),)),
        "out_weights": normal_values(splits[4], (N_SECTION, C, C), C ** -0.5, 0.25, ((0, 4),)),
        "norm_gains": jnp.clip(1.0 + 0.18 * jax.random.normal(splits[5], (N_SECTION, C), jnp.float32), 0.099609375, 1.8984375).astype(jnp.bfloat16),
        "quant_weight": normal_values(splits[6], (C, BITS), C ** -0.5, 0.25),
        "quant_bias": normal_values(splits[7], (BITS,), 1.0, 3.0, (), jnp.float32),
        "post_weight": normal_values(splits[8], (BITS, C), BITS ** -0.5, 1.5),
    }


norm_eps = 1e-06
quant_section = 1

def run_block(current, tap_set, out_weight, gain_row):
    clip_count, row_count, channels = current.shape
    widened = current.astype(jnp.float32)
    scale = lax.rsqrt(lax.optimization_barrier(jnp.mean(widened * widened, axis=-1, keepdims=True)) + norm_eps)
    normed = (widened * scale * gain_row.astype(jnp.float32)).astype(jnp.bfloat16)
    flat = normed.reshape(-1, channels)
    mixed = jnp.zeros((clip_count, row_count, channels), jnp.float32)
    for k in range(tap_set.shape[0]):
        product = jnp.dot(flat, tap_set[k], preferred_element_type=jnp.float32).reshape(clip_count, row_count, channels)
        moved = jnp.pad(product, ((0, 0), (k * SPATIAL, 0), (0, 0)))[:, :row_count]
        mixed = mixed + moved
    activated = jax.nn.silu(mixed).astype(jnp.bfloat16)
    update = jnp.dot(activated.reshape(-1, channels), out_weight, preferred_element_type=jnp.float32)
    return (widened + update.reshape(clip_count, row_count, channels)).astype(jnp.bfloat16)

def quantize(current, quant_weight, quant_bias, post_weight):
    channels = current.shape[-1]
    logits = jnp.dot(current.reshape(-1, channels), quant_weight, preferred_element_type=jnp.float32) + quant_bias
    bit_prob = jax.nn.sigmoid(4.0 * logits)
    codes = (2.0 * bit_prob - 1.0).astype(jnp.bfloat16)
    quantized = jnp.dot(codes, post_weight, preferred_element_type=jnp.float32).astype(jnp.bfloat16)
    bit_sums = lax.optimization_barrier(jnp.sum(bit_prob, axis=0))
    entropy_sum = -jnp.sum(bit_prob * jax.nn.log_sigmoid(4.0 * logits) + (1.0 - bit_prob) * jax.nn.log_sigmoid(-4.0 * logits))
    return (quantized.reshape(current.shape), bit_sums, entropy_sum)

def squared_error(decoded, source):
    differ = decoded.astype(jnp.float32) - source.astype(jnp.float32)
    return lax.optimization_barrier(jnp.mean(differ * differ, axis=-1))

def final_entropy(bit_buffer, entropy_buffer, batch_order, rows_total):
    marginal = bit_buffer / rows_total
    sample_entropy = entropy_buffer / rows_total
    averaged = jnp.zeros_like(marginal)
    running = marginal[batch_order[0]]
    for t in range(batch_order.shape[0]):
        if t > 0:
            running = 0.5 * running + 0.5 * marginal[batch_order[t]]
        averaged = averaged.at[batch_order[t]].set(running)
    smoothed = 0.05 + 0.9 * averaged
    code_entropy = -lax.optimization_barrier(jnp.sum(smoothed * jnp.log(smoothed) + (1.0 - smoothed) * jnp.log(1.0 - smoothed), axis=-1))
    return sample_entropy - code_entropy

def reference(clip_pool, clip_index, batch_order, tap_weights, out_weights, norm_gains, quant_weight, quant_bias, post_weight):
    replica = jnp.arange(CL_ALL, dtype=jnp.int32) // CLIPS
    error_list = []
    bit_list = []
    entropy_list = []
    for j in range(MB):
        chosen = (replica * POOL + clip_index[j]).astype(jnp.int32)
        source = clip_pool[chosen]
        current = source
        for s in range(N_SECTION):
            current = run_block(current, tap_weights[s], out_weights[s], norm_gains[s])
            if s == quant_section:
                current, bit_sums, entropy_sum = quantize(current, quant_weight, quant_bias, post_weight)
                bit_list.append(bit_sums)
                entropy_list.append(entropy_sum)
        error_list.append(squared_error(current, source))
    rows_total = float(CL_ALL * ROWS)
    losses = final_entropy(jnp.stack(bit_list), jnp.stack(entropy_list), batch_order, rows_total)
    return (jnp.stack(error_list), losses)
```

```python
import functools

import jax
import jax.numpy as jnp
from jax import lax
from jax.experimental import pallas as pl
from jax.experimental.pallas import tpu as pltpu
from jax.sharding import Mesh
from jax.sharding import PartitionSpec as P


DP = ("dp_0", "dp_1", "dp_2")
MESH = pl.DeviceIdType.MESH
F32 = jnp.float32
BF16 = jnp.bfloat16
C = 512
BITS = 18
CLIPS = 4
ROWS = 256
SPATIAL = 64
GROUP = CLIPS * ROWS
NORM_EPS = 1e-06
ROWS_TOTAL = 128.0 * 256.0


def dot(a, b):
    return jnp.dot(a, b, preferred_element_type=F32)


def silu(u):
    return 0.5 * u * (1.0 + jnp.tanh(0.5 * u))


def rows_of(value, first, count):
    parts = value.reshape(CLIPS, -1, value.shape[-1])
    return parts[:, first : first + count].reshape(CLIPS * count, value.shape[-1])


def normalize(v, gain):
    wide = v.astype(F32)
    mean = jnp.mean(wide * wide, axis=-1, keepdims=True)
    return (wide * lax.rsqrt(mean + NORM_EPS) * gain).astype(BF16)


def taps(n, weight):
    p0 = dot(n, weight(0)).reshape(CLIPS, ROWS, C)
    p1 = dot(rows_of(n, 0, ROWS - SPATIAL), weight(1)).reshape(CLIPS, ROWS - SPATIAL, C)
    p2 = dot(rows_of(n, 0, ROWS - 2 * SPATIAL), weight(2)).reshape(CLIPS, ROWS - 2 * SPATIAL, C)
    mixed = jnp.concatenate(
        [
            p0[:, :SPATIAL],
            p0[:, SPATIAL : 2 * SPATIAL] + p1[:, :SPATIAL],
            p0[:, 2 * SPATIAL :] + p1[:, SPATIAL:] + p2,
        ],
        axis=1,
    )
    return mixed.reshape(GROUP, C)


def kernel(
    index_ref, order_ref, pool_hbm, taps_hbm, out_hbm, gains_hbm, qw_hbm, qb_hbm, pw_hbm,
    error_ref, loss_ref,
    pool, wts, gains, act, acc, qw, qb, pw, qwp, pwp, stat1, stat2,
    lsem, xs, xr, gs, gr, rs, rr, ds, dr, s1s, s1r, s2s, s2r,
):
    x = lax.axis_index("section")
    y = lax.axis_index("dp_0")
    z = lax.axis_index("dp_1")
    c = lax.axis_index("dp_2")
    q = y * (1 - c) + z * c

    def xpeer(d):
        return (lax.rem(x + d, 4), y, z, c)

    def ring(d):
        return (x, lax.rem(y + d * (1 - c), 4), lax.rem(z + d * c, 4), c)

    def plane(dy, dz):
        return (x, lax.rem(y + dy, 4), lax.rem(z + dz, 4), c)

    def other(d, e):
        return (lax.rem(x + d, 4), y, z, lax.rem(c + e, 2))

    sibling = other(0, 1)
    planes = [(dy, dz) for dy in range(4) for dz in range(4) if dy or dz]
    others = [(d, e) for d in range(4) for e in range(2) if d or e]

    loads = [
        (taps_hbm.at[0], wts.at[x, pl.ds(0, 3)]),
        (out_hbm.at[0], wts.at[x, 3]),
        (gains_hbm, gains.at[x]),
        (pool_hbm, pool),
        (qw_hbm, qw),
        (qb_hbm, qb),
        (pw_hbm, pw),
    ]
    loads = [pltpu.make_async_copy(a, b, lsem.at[i]) for i, (a, b) in enumerate(loads)]
    for load in loads:
        load.start()
    barrier = pltpu.get_barrier_semaphore()
    for dy, dz in planes:
        pl.semaphore_signal(barrier, inc=1, device_id=plane(dy, dz), device_id_type=MESH)
    for d, e in others:
        pl.semaphore_signal(barrier, inc=1, device_id=other(d, e), device_id_type=MESH)
    pl.semaphore_wait(barrier, len(planes) + len(others))
    for load in loads[:3]:
        load.wait()

    def remote(ref, send, recv, device):
        return pltpu.make_async_remote_copy(
            ref, ref, send, recv, device_id=device, device_id_type=MESH
        )

    def quarter(b, m, owner):
        return wts.at[b, m, pl.ds(pl.multiple_of(c * 256 + owner * 64, 64), 64)]

    def xcopy(b, m, d):
        return remote(quarter(b, m, q), xs.at[m, d - 1], xr.at[b, m], xpeer(d))

    def gcopy(b, d):
        return remote(gains.at[b], gs.at[d - 1], gr.at[b], xpeer(d))

    def rcopy(b, m, d, owner):
        return remote(quarter(b, m, owner), rs.at[b, m, d - 1], rr.at[b, m, d - 1], ring(d))

    def dcopy(b, m, h):
        ref = wts.at[b, m, pl.ds(pl.multiple_of(h * 256, 256), 256)]
        return remote(ref, ds.at[b, m], dr.at[b, m], sibling)

    def own(m, *distances):
        for d in distances:
            xcopy(x, m, d).start()

    for d in (1, 3, 2):
        gcopy(x, d).start()

    @pl.when(x == 0)
    def _():
        for m in range(4):
            own(m, 1, 3, 2)

    @pl.when(x == 1)
    def _():
        for m in range(4):
            own(m, 3)

    def X(b, m):
        @pl.when(x != b)
        def _():
            xcopy(b, m, 1).wait_recv()
            for d in (1, 3, 2):
                rcopy(b, m, d, q).start()

        if b == 0:

            @pl.when(x == 1)
            def _():
                own(m, 1, 2)

            @pl.when(x == 2)
            def _():
                own(m, 3, 1, 2)

        if b == 1:

            @pl.when(x == 3)
            def _():
                own(m, 1, 3, 2)

    def R(b, m):
        @pl.when(x != b)
        def _():
            for d in (1, 3, 2):
                rcopy(b, m, d, lax.rem(q + 4 - d, 4)).wait_recv()
            dcopy(b, m, c).start()

    def D(b, m):
        @pl.when(x != b)
        def _():
            dcopy(b, m, 1 - c).wait_recv()
            if m == 0:
                gcopy(b, 1).wait_recv()

    def group(g):
        return pl.ds(g * GROUP, GROUP)

    def gain(b):
        return gains[b].astype(F32)

    def source(i, k):
        return pool[index_ref[2 * x + i, k]]

    def weight(b):
        return lambda m: wts[b, m]

    def c0(m, g):
        def part(n, skip):
            product = dot(rows_of(n, 0, ROWS - skip), wts[0, m]).reshape(CLIPS, ROWS - skip, C)
            for k in range(CLIPS):
                at = pl.ds(g * GROUP + k * ROWS + skip, ROWS - skip)
                acc[at, :] = acc[at, :] + product[k]

        if m == 0:
            for k in range(CLIPS):
                at = pl.ds(g * GROUP + k * ROWS, ROWS)
                act[at, :] = normalize(source(g, k), gain(0))
            acc[group(g), :] = dot(act[group(g), :], wts[0, 0])
        elif m < 3:
            part(act[group(g), :], m * SPATIAL)
        else:
            v = jnp.concatenate([source(g, k) for k in range(CLIPS)], axis=0)
            a = silu(acc[group(g), :]).astype(BF16)
            act[group(g), :] = (v.astype(F32) + dot(a, wts[0, 3])).astype(BF16)

    def cb(b, g):
        v = act[group(g), :]
        n = normalize(v, gain(b))
        a = silu(taps(n, weight(b))).astype(BF16)
        act[group(g), :] = (v.astype(F32) + dot(a, wts[b, 3])).astype(BF16)

    lane = lax.broadcasted_iota(jnp.int32, (8, 128), 1)
    row = lax.broadcasted_iota(jnp.int32, (8, 128), 0)

    def quantize(g):
        t = 4.0 * (dot(act[group(g), :], qwp[...]) + qb[...])
        codes = jnp.tanh(0.5 * t)
        act[group(g), :] = dot(codes.astype(BF16), pwp[...]).astype(BF16)
        size = jnp.abs(t)
        e = jnp.exp(-size)
        entropy = jnp.log(1.0 + e) + size * e / (1.0 + e)
        bit = jnp.sum(0.5 * (1.0 + codes), axis=0, keepdims=True)
        ent = jnp.sum(entropy, axis=0, keepdims=True)
        ent = jnp.sum(jnp.where(lane[:1] < BITS, ent, 0.0), axis=1, keepdims=True)
        both = jnp.where(lane[:1] < BITS, bit, jnp.where(lane[:1] == BITS, ent, 0.0))
        return jnp.where(row == 2 * x + g, both, 0.0)

    def s1copy(dy, dz, sy, sz):
        k = dy * 4 + dz
        ref = stat1.at[sy * 4 + sz]
        return remote(ref, s1s.at[k], s1r.at[k], plane(dy, dz))

    def s2copy(d, e, sx, sc):
        k = d * 2 + e
        ref = stat2.at[sx * 2 + sc]
        return remote(ref, s2s.at[k], s2r.at[k], other(d, e))

    def errors(g):
        for k in range(CLIPS):
            at = pl.ds(g * GROUP + k * ROWS, ROWS)
            differ = act[at, :].astype(F32) - source(g, k).astype(F32)
            square = differ * differ
            part = square[:, :128] + square[:, 128:256] + square[:, 256:384] + square[:, 384:]
            total = jnp.sum(part.T, axis=0, keepdims=True)
            error_ref[g, k : k + 1, :] = total * (1.0 / C)

    X(0, 0)
    X(0, 1)
    R(0, 0)
    X(0, 2)
    D(0, 0)
    loads[3].wait()
    c0(0, 0)
    R(0, 1)
    X(0, 3)
    c0(0, 1)
    X(1, 0)
    D(0, 1)
    c0(1, 0)
    R(0, 2)
    c0(1, 1)
    X(1, 1)
    D(0, 2)
    c0(2, 0)
    R(0, 3)
    c0(2, 1)
    X(1, 2)
    D(0, 3)
    c0(3, 0)
    R(1, 0)
    X(1, 3)
    c0(3, 1)
    for load in loads[4:]:
        load.wait()
    qwp[...] = jnp.zeros_like(qwp)
    pwp[...] = jnp.zeros_like(pwp)
    qwp[:, 0:BITS] = qw[...]
    pwp[0:BITS, :] = pw[...]
    R(1, 1)
    X(2, 0)
    D(1, 0)
    R(1, 2)
    D(1, 1)
    X(2, 1)
    R(1, 3)
    D(1, 2)
    X(2, 2)
    D(1, 3)
    cb(1, 0)
    R(2, 0)
    R(2, 1)
    X(2, 3)
    cb(1, 1)
    R(2, 2)
    D(2, 0)
    stats = quantize(0) + quantize(1)
    stat1[y * 4 + z] = stats
    R(2, 3)
    D(2, 1)
    X(3, 0)
    X(3, 1)
    D(2, 2)
    D(2, 3)
    cb(2, 0)
    for dy, dz in planes:
        s1copy(dy, dz, y, z).start()
    X(3, 2)
    R(3, 0)
    X(3, 3)
    R(3, 1)
    cb(2, 1)
    for dy, dz in planes:
        s1copy(dy, dz, lax.rem(y + 4 - dy, 4), lax.rem(z + 4 - dz, 4)).wait_recv()
    total = stat1[0]
    for k in range(1, 16):
        total = total + stat1[k]
    stat2[x * 2 + c] = total
    R(3, 2)
    D(3, 0)
    R(3, 3)
    D(3, 1)
    D(3, 2)
    D(3, 3)
    for d, e in others:
        s2copy(d, e, x, c).start()
    cb(3, 0)
    errors(0)
    cb(3, 1)
    errors(1)

    for d, e in others:
        s2copy(d, e, lax.rem(x + 4 - d, 4), lax.rem(c + 2 - e, 2)).wait_recv()
    total = stat2[0]
    for k in range(1, 8):
        total = total + stat2[k]
    mean = total / ROWS_TOTAL
    averaged = jnp.zeros((8, 128), F32)
    running = None
    for t in range(8):
        chosen = row == order_ref[t]
        marginal = jnp.sum(jnp.where(chosen, mean, 0.0), axis=0, keepdims=True)
        running = marginal if t == 0 else 0.5 * running + 0.5 * marginal
        averaged = jnp.where(chosen, running, averaged)
    smoothed = 0.05 + 0.9 * averaged
    smoothed = jnp.where(lane < BITS, smoothed, 0.5)
    terms = smoothed * jnp.log(smoothed) + (1.0 - smoothed) * jnp.log(1.0 - smoothed)
    terms = jnp.where(lane < BITS, terms, jnp.where(lane == BITS, mean, 0.0))
    loss_ref[...] = jnp.sum(terms, axis=1, keepdims=True) + jnp.zeros((8, 128), F32)

    for d in (1, 3, 2):
        gcopy(x, d).wait_send()
        for m in range(4):
            xcopy(x, m, d).wait_send()
    for b in range(4):

        @pl.when(x != b)
        def _():
            for m in range(4):
                for d in (1, 3, 2):
                    rcopy(b, m, d, q).wait_send()
                dcopy(b, m, c).wait_send()

    for dy, dz in planes:
        s1copy(dy, dz, y, z).wait_send()
    for d, e in others:
        s2copy(d, e, x, c).wait_send()


def on_device(
    clip_pool, clip_index, batch_order, tap_weights, out_weights, norm_gains,
    quant_weight, quant_bias, post_weight,
):
    any_space = pl.BlockSpec(memory_space=pl.ANY)
    smem = pl.BlockSpec(memory_space=pltpu.SMEM)
    vmem = pl.BlockSpec(memory_space=pltpu.VMEM)
    dma = pltpu.SemaphoreType.DMA
    bias = jnp.zeros((1, 128), F32).at[0, :BITS].set(quant_bias)
    error, loss = pl.pallas_call(
        kernel,
        out_shape=(
            jax.ShapeDtypeStruct((2, CLIPS, ROWS), F32),
            jax.ShapeDtypeStruct((8, 128), F32),
        ),
        in_specs=[smem, smem] + [any_space] * 7,
        out_specs=(vmem, vmem),
        scratch_shapes=[
            pltpu.VMEM((32, ROWS, C), BF16),
            pltpu.VMEM((4, 4, C, C), BF16),
            pltpu.VMEM((4, 1, C), BF16),
            pltpu.VMEM((2 * GROUP, C), BF16),
            pltpu.VMEM((2 * GROUP, C), F32),
            pltpu.VMEM((C, BITS), BF16),
            pltpu.VMEM((1, 128), F32),
            pltpu.VMEM((BITS, C), BF16),
            pltpu.VMEM((C, 128), BF16),
            pltpu.VMEM((128, C), BF16),
            pltpu.VMEM((16, 8, 128), F32),
            pltpu.VMEM((8, 8, 128), F32),
            dma((7,)),
            dma((4, 3)),
            dma((4, 4)),
            dma((3,)),
            dma((4,)),
            dma((4, 4, 3)),
            dma((4, 4, 3)),
            dma((4, 4)),
            dma((4, 4)),
            dma((16,)),
            dma((16,)),
            dma((8,)),
            dma((8,)),
        ],
        compiler_params=pltpu.CompilerParams(
            collective_id=0, has_side_effects=True, vmem_limit_bytes=60 * 2**20
        ),
    )(
        clip_index, batch_order, clip_pool, tap_weights, out_weights, norm_gains,
        quant_weight, bias, post_weight,
    )
    return error, loss[:, 0]


def solution(mesh):
    torus = Mesh(
        mesh.devices.reshape(mesh.shape["section"], 4, 4, 2), ("section", "dp_0", "dp_1", "dp_2")
    )
    return jax.shard_map(
        on_device,
        mesh=torus,
        in_specs=(
            P(DP, None, None),
            P(None, DP),
            P(),
            P("section", None, None, None),
            P("section", None, None),
            P("section", None),
            P(),
            P(),
            P(),
        ),
        out_specs=(P("section", DP, None), P()),
        check_vma=False,
    )
```

```python
import functools

import jax
import jax.numpy as jnp
from jax import lax
from jax.experimental import pallas as pl
from jax.experimental.pallas import tpu as pltpu
from jax.sharding import Mesh
from jax.sharding import PartitionSpec as P


DP = ("dp_0", "dp_1", "dp_2")
MESH = pl.DeviceIdType.MESH
F32 = jnp.float32
BF16 = jnp.bfloat16
C = 512
BITS = 18
PAD = 32
CLIPS = 4
ROWS = 256
SPATIAL = 64
GROUP = CLIPS * ROWS
NORM_EPS = 1e-06
ROWS_TOTAL = 128.0 * 256.0
DIRECT = (0, 2)

SCHEDULE = (
    ("V", 0), ("X", 0, 0), ("Y", 0), ("V", 1), ("V", 2), ("X", 0, 1), ("Y", 1), ("V", 3), ("X", 0, 2),
    ("Y", 2), ("X", 0, 3), ("Y", 3), ("R", 0, 0), ("X", 1, 0), ("X", 1, 1), ("Z", 0), ("Z", 1), ("R", 0, 1),
    ("E", 0, 0), ("pool",), ("cs", 0, 0, 0), ("cs", 0, 0, 1), ("R", 0, 2), ("X", 1, 2), ("Z", 2), ("Z", 3),
    ("E", 0, 1), ("cs", 0, 1, 0), ("cs", 0, 1, 1), ("R", 0, 3), ("X", 1, 3), ("E", 0, 2), ("cs", 0, 2, 0),
    ("X", 2, 0), ("cs", 0, 2, 1), ("R", 1, 0), ("E", 0, 3), ("cs", 0, 3, 0), ("X", 2, 1), ("cs", 0, 3, 1),
    ("prep",), ("R", 1, 1), ("X", 2, 2), ("L", 0), ("E", 1, 0), ("cs", 1, 0, 0), ("R", 1, 2), ("X", 2, 3),
    ("cs", 1, 0, 1), ("E", 1, 1), ("cs", 1, 1, 0), ("R", 1, 3), ("cs", 1, 1, 1), ("E", 1, 2), ("cs", 1, 2, 0),
    ("R", 2, 0), ("cs", 1, 2, 1), ("E", 1, 3), ("cs", 1, 3, 0), ("R", 2, 1), ("cs", 1, 3, 1), ("R", 2, 2),
    ("quant",), ("s1send",), ("R", 2, 3), ("L", 1), ("E", 2, 0), ("E", 2, 1), ("E", 2, 2), ("E", 2, 3),
    ("cb", 2, 0), ("cb", 2, 1), ("s1take",), ("s2send",), ("L", 2), ("cb", 3, 0), ("err", 0), ("cb", 3, 1),
    ("err", 1),
)


def dot(a, b):
    return jnp.dot(a, b, preferred_element_type=F32)


def dot_t(a, b):
    return lax.dot_general(a, b, (((1,), (1,)), ((), ())), preferred_element_type=F32)


def silu(u):
    return 0.5 * u * (1.0 + jnp.tanh(0.5 * u))


def rows_of(value, first, count):
    parts = value.reshape(CLIPS, -1, value.shape[-1])
    return parts[:, first : first + count].reshape(CLIPS * count, value.shape[-1])


def normalize(v, gain):
    wide = v.astype(F32)
    mean = jnp.mean(wide * wide, axis=-1, keepdims=True)
    return (wide * lax.rsqrt(mean + NORM_EPS) * gain).astype(BF16)


def taps(n, weight):
    p0 = dot(n, weight(0)).reshape(CLIPS, ROWS, C)
    p1 = dot(rows_of(n, 0, ROWS - SPATIAL), weight(1)).reshape(CLIPS, ROWS - SPATIAL, C)
    p2 = dot(rows_of(n, 0, ROWS - 2 * SPATIAL), weight(2)).reshape(CLIPS, ROWS - 2 * SPATIAL, C)
    mixed = jnp.concatenate(
        [
            p0[:, :SPATIAL],
            p0[:, SPATIAL : 2 * SPATIAL] + p1[:, :SPATIAL],
            p0[:, 2 * SPATIAL :] + p1[:, SPATIAL:] + p2,
        ],
        axis=1,
    )
    return mixed.reshape(GROUP, C)


def kernel(
    index_hbm, order_hbm, pool_hbm, taps_hbm, out_hbm, gains_hbm, qw_hbm, qb_hbm, pw_hbm,
    error_hbm, loss_hbm,
    pool, wts, gains, act, nrm, acc, index_ref, order_ref, qb, qw, pw, qwp, pwp, stat1, stat2, error_ref, loss_ref,
    lsem, osem, xs, xr, ys, zs, gs, gr, rs, rr, ds, dr, s1s, s1r, s2s, s2r,
):
    x = lax.axis_index("section")
    y = lax.axis_index("dp_0")
    z = lax.axis_index("dp_1")
    c = lax.axis_index("dp_2")
    q = y * (1 - c) + z * c

    def xpeer(d):
        return (lax.rem(x + d, 4), y, z, c)

    def ring(d):
        return (x, lax.rem(y + d * (1 - c), 4), lax.rem(z + d * c, 4), c)

    def plane(dy, dz):
        return (x, lax.rem(y + dy, 4), lax.rem(z + dz, 4), c)

    def other(d, e):
        return (lax.rem(x + d, 4), y, z, lax.rem(c + e, 2))

    sibling = other(0, 1)
    near = [(d, 0) for d in (1, 2, 3)] + [(0, d) for d in (1, 2, 3)]
    planes = [(dy, dz) for dy in range(4) for dz in range(4) if dy or dz]
    others = [(d, e) for d in range(4) for e in range(2) if d or e]

    barrier = pltpu.get_barrier_semaphore()
    for dy, dz in near:
        pl.semaphore_signal(barrier, inc=1, device_id=plane(dy, dz), device_id_type=MESH)
    for d, e in others:
        pl.semaphore_signal(barrier, inc=1, device_id=other(d, e), device_id_type=MESH)
    loads = [
        (taps_hbm.at[0], wts.at[x, pl.ds(0, 3)]),
        (out_hbm.at[0], wts.at[x, 3]),
        (gains_hbm, gains.at[x]),
        (index_hbm, index_ref),
        (pool_hbm, pool),
        (order_hbm, order_ref),
        (qb_hbm, qb),
        (qw_hbm, qw),
        (pw_hbm, pw),
    ]
    loads = [pltpu.make_async_copy(a, b, lsem.at[i]) for i, (a, b) in enumerate(loads)]
    for load in loads:
        load.start()
    with jax.named_scope("barrier"):
        pl.semaphore_wait(barrier, len(near) + len(others))
    for load in loads[:3]:
        load.wait()

    def remote(ref, send, recv, device):
        return pltpu.make_async_remote_copy(
            ref, ref, send, recv, device_id=device, device_id_type=MESH
        )

    def quarter(b, m, owner):
        return wts.at[b, m, pl.ds(pl.multiple_of(c * 256 + owner * 64, 64), 64)]

    def xcopy(b, m, d):
        return remote(quarter(b, m, q), xs.at[m, d // 2], xr.at[b, m], xpeer(d))

    def relay(m):
        b = 3 - x
        return remote(quarter(b, m, q), ys.at[m], xr.at[b, m], xpeer(1 + 2 * lax.rem(x, 2)))

    def across(m):
        return remote(quarter(0, m, q), zs.at[m], xr.at[0, m], xpeer(2))

    def gcopy(b, d):
        return remote(gains.at[b], gs.at[d - 1], gr.at[b], xpeer(d))

    def rcopy(b, m, d, owner):
        return remote(quarter(b, m, owner), rs.at[b, m, d - 1], rr.at[b, m, d - 1], ring(d))

    def dcopy(b, m, h):
        ref = wts.at[b, m, pl.ds(pl.multiple_of(h * 256, 256), 256)]
        return remote(ref, ds.at[b, m], dr.at[b, m], sibling)

    def foreign(f):
        return jnp.where(x <= f, f + 1, f)

    def own(m, d):
        xcopy(x, m, d).start()

    for m in range(4):

        @pl.when(x == 0)
        def _():
            own(m, 1)
            own(m, 3)
            if m in DIRECT:
                across(m).start()

        @pl.when(x == 1)
        def _():
            own(m, 3)
            own(m, 1)

        @pl.when(x == 2)
        def _():
            own(m, 3)

        @pl.when(x == 3)
        def _():
            own(m, 1)

    for d in (1, 3, 2):
        gcopy(x, d).start()

    def take(f, m):
        xcopy(foreign(f), m, 1).wait_recv()

    def V(m):
        @pl.when(x == 2)
        def _():
            take(1, m)
            relay(m).start()
            if m == 3:
                for k in range(4):
                    own(k, 1)

    def Y(m):
        @pl.when(x == 1)
        def _():
            take(1, m)
            relay(m).start()

    def Z(m):
        @pl.when(x == 0)
        def _():
            take(2, m)
            relay(m).start()

    def X(f, m):
        if f == 0:
            take(f, m)

            @pl.when(x == 3)
            def _():
                if m not in DIRECT:
                    relay(m).start()
                if m == 3:
                    for k in range(4):
                        own(k, 3)

        elif f == 1:

            @pl.when((x == 0) | (x == 3))
            def _():
                take(f, m)
        else:

            @pl.when(x > 0)
            def _():
                take(f, m)

        for d in (1, 3, 2):
            rcopy(foreign(f), m, d, q).start()

    def R(f, m):
        for d in (1, 3, 2):
            rcopy(foreign(f), m, d, lax.rem(q + 4 - d, 4)).wait_recv()
        dcopy(foreign(f), m, c).start()

    def landed(f, m):
        dcopy(foreign(f), m, 1 - c).wait_recv()
        if m == 0:
            gcopy(foreign(f), 1).wait_recv()

    def E(f, m):
        @pl.when(x > f)
        def _():
            landed(f, m)

    def L(f):
        @pl.when(x <= f)
        def _():
            for m in range(4):
                landed(f, m)

    def group(g):
        return pl.ds(g * GROUP, GROUP)

    def gain(b):
        return gains[b].astype(F32)

    def source(i, k):
        return pool[index_ref[k, 2 * x + i]]

    def weight(b):
        return lambda m: wts[b, m]

    def cs(b, m, g):
        def part(n, skip):
            product = dot(rows_of(n, 0, ROWS - skip), wts[b, m]).reshape(CLIPS, ROWS - skip, C)
            for k in range(CLIPS):
                at = pl.ds(g * GROUP + k * ROWS + skip, ROWS - skip)
                acc[at, :] = acc[at, :] + product[k]

        if m == 0 or m == 3:
            if b == 0:
                v = jnp.concatenate([source(g, k) for k in range(CLIPS)], axis=0)
            else:
                v = act[group(g), :]
        if m == 0:
            n = normalize(v, gain(b))
            nrm[group(g), :] = n
            acc[group(g), :] = dot(n, wts[b, 0])
        elif m < 3:
            part(nrm[group(g), :], m * SPATIAL)
        else:
            a = silu(acc[group(g), :]).astype(BF16)
            act[group(g), :] = (v.astype(F32) + dot(a, wts[b, 3])).astype(BF16)

    def cb(b, g):
        v = act[group(g), :]
        n = normalize(v, gain(b))
        a = silu(taps(n, weight(b))).astype(BF16)
        act[group(g), :] = (v.astype(F32) + dot(a, wts[b, 3])).astype(BF16)

    lane = lax.broadcasted_iota(jnp.int32, (8, 128), 1)
    row = lax.broadcasted_iota(jnp.int32, (8, 128), 0)

    def quantize(g):
        t = 4.0 * (dot_t(qwp[...], act[group(g), :]) + bias())
        codes = jnp.tanh(0.5 * t)
        back = lax.dot_general(
            codes.astype(BF16), pwp[...], (((0,), (0,)), ((), ())), preferred_element_type=F32
        )
        act[group(g), :] = back.astype(BF16)
        size = jnp.abs(t)
        e = jnp.exp(-size)
        entropy = jnp.log(1.0 + e) + size * e / (1.0 + e)
        bit = jnp.sum(0.5 * (1.0 + codes), axis=1, keepdims=True)
        ent = jnp.sum(entropy, axis=1, keepdims=True)
        at = lax.broadcasted_iota(jnp.int32, (PAD, 128), 0)
        col = lax.broadcasted_iota(jnp.int32, (PAD, 128), 1)
        bit = jnp.sum(jnp.where((at == col) & (col < BITS), bit, 0.0), axis=0, keepdims=True)
        ent = jnp.sum(jnp.where((at < BITS) & (col == BITS), ent, 0.0), axis=0, keepdims=True)
        return jnp.where(row == 2 * x + g, bit + ent, 0.0)

    def bias():
        at = lax.broadcasted_iota(jnp.int32, (PAD, 1), 0)
        value = jnp.zeros((PAD, 1), F32)
        for k in range(BITS):
            value = jnp.where(at == k, qb[k], value)
        return value

    def s1copy(dy, dz, sy, sz):
        k = dy * 4 + dz
        ref = stat1.at[sy * 4 + sz]
        return remote(ref, s1s.at[k], s1r.at[k], plane(dy, dz))

    def s2copy(d, e, sx, sc):
        k = d * 2 + e
        ref = stat2.at[sx * 2 + sc]
        return remote(ref, s2s.at[k], s2r.at[k], other(d, e))

    stored = [
        pltpu.make_async_copy(error_ref.at[g], error_hbm.at[g], osem.at[g]) for g in range(2)
    ] + [pltpu.make_async_copy(loss_ref, loss_hbm, osem.at[2])]

    def errors(g):
        for k in range(CLIPS):
            at = pl.ds(g * GROUP + k * ROWS, ROWS)
            differ = act[at, :].astype(F32) - source(g, k).astype(F32)
            square = differ * differ
            part = square[:, :128] + square[:, 128:256] + square[:, 256:384] + square[:, 384:]
            total = jnp.sum(part.T, axis=0, keepdims=True)
            error_ref[g, k : k + 1, :] = total * (1.0 / C)
        stored[g].start()

    def pool_ready():
        loads[3].wait()
        loads[4].wait()

    def quantizers():
        for load in loads[5:]:
            load.wait()
        qwp[...] = jnp.zeros_like(qwp)
        pwp[...] = jnp.zeros_like(pwp)
        qwp[0:BITS, :] = qw[...]
        pwp[0:BITS, :] = pw[...]

    def quantize_both():
        stat1[y * 4 + z] = quantize(0) + quantize(1)

    def s1send():
        for dy, dz in planes:
            s1copy(dy, dz, y, z).start()

    def s1take():
        for dy, dz in planes:
            s1copy(dy, dz, lax.rem(y + 4 - dy, 4), lax.rem(z + 4 - dz, 4)).wait_recv()
        total = stat1[0]
        for k in range(1, 16):
            total = total + stat1[k]
        stat2[x * 2 + c] = total

    def s2send():
        for d, e in others:
            s2copy(d, e, x, c).start()

    steps = {
        "X": X, "Y": Y, "V": V, "Z": Z, "R": R, "E": E, "L": L, "cs": cs, "cb": cb, "err": errors, "pool": pool_ready,
        "prep": quantizers, "quant": quantize_both, "s1send": s1send, "s1take": s1take, "s2send": s2send,
    }
    for name, *numbers in SCHEDULE:
        with jax.named_scope("_".join(map(str, [name, *numbers]))):
            steps[name](*numbers)

    with jax.named_scope("s2take"):
        for d, e in others:
            s2copy(d, e, lax.rem(x + 4 - d, 4), lax.rem(c + 2 - e, 2)).wait_recv()
    with jax.named_scope("loss"):
        total = stat2[0]
        for k in range(1, 8):
            total = total + stat2[k]
        mean = total / ROWS_TOTAL
        averaged = jnp.zeros((8, 128), F32)
        running = None
        for t in range(8):
            chosen = row == order_ref[t]
            marginal = jnp.sum(jnp.where(chosen, mean, 0.0), axis=0, keepdims=True)
            running = marginal if t == 0 else 0.5 * running + 0.5 * marginal
            averaged = jnp.where(chosen, running, averaged)
        smoothed = 0.05 + 0.9 * averaged
        smoothed = jnp.where(lane < BITS, smoothed, 0.5)
        terms = smoothed * jnp.log(smoothed) + (1.0 - smoothed) * jnp.log(1.0 - smoothed)
        terms = jnp.where(lane < BITS, terms, jnp.where(lane == BITS, mean, 0.0))
        loss = jnp.sum(terms, axis=1, keepdims=True)
        loss_ref[...] = jnp.sum(jnp.where(row == lane, loss, 0.0), axis=0, keepdims=True)

    stored[2].start()

    for d in (1, 3, 2):
        gcopy(x, d).wait_send()
    for m in range(4):
        xcopy(x, m, 1).wait_send()
        xcopy(x, m, 3).wait_send()
        if m in DIRECT:

            @pl.when(x == 0)
            def _():
                across(m).wait_send()

            @pl.when(x < 3)
            def _():
                relay(m).wait_send()
        else:
            relay(m).wait_send()
        for f in range(3):
            for d in (1, 3, 2):
                rcopy(foreign(f), m, d, q).wait_send()
            dcopy(foreign(f), m, c).wait_send()
    for dy, dz in planes:
        s1copy(dy, dz, y, z).wait_send()
    for d, e in others:
        s2copy(d, e, x, c).wait_send()
    for copy in stored:
        copy.wait()


def finish(error_in, loss_in, error_out, loss_out):
    error_out[...] = error_in[...]
    loss_out[...] = loss_in[:, 0:8]


def on_device(
    clip_pool, clip_index, batch_order, tap_weights, out_weights, norm_gains,
    quant_weight, quant_bias, post_weight,
):
    any_space = pl.BlockSpec(memory_space=pl.ANY)
    vmem = pl.BlockSpec(memory_space=pltpu.VMEM)
    dma = pltpu.SemaphoreType.DMA
    error, loss = pl.pallas_call(
        kernel,
        out_shape=(
            jax.ShapeDtypeStruct((2, CLIPS, ROWS), F32),
            jax.ShapeDtypeStruct((1, 128), F32),
        ),
        in_specs=[any_space] * 9,
        out_specs=(any_space, any_space),
        scratch_shapes=[
            pltpu.VMEM((32, ROWS, C), BF16),
            pltpu.VMEM((4, 4, C, C), BF16),
            pltpu.VMEM((4, 1, C), BF16),
            pltpu.VMEM((2 * GROUP, C), BF16),
            pltpu.VMEM((2 * GROUP, C), BF16),
            pltpu.VMEM((2 * GROUP, C), F32),
            pltpu.SMEM((CLIPS, 8), jnp.int32),
            pltpu.SMEM((8,), jnp.int32),
            pltpu.SMEM((BITS,), F32),
            pltpu.VMEM((BITS, C), BF16),
            pltpu.VMEM((BITS, C), BF16),
            pltpu.VMEM((PAD, C), BF16),
            pltpu.VMEM((PAD, C), BF16),
            pltpu.VMEM((16, 8, 128), F32),
            pltpu.VMEM((8, 8, 128), F32),
            pltpu.VMEM((2, CLIPS, ROWS), F32),
            pltpu.VMEM((1, 128), F32),
            dma((9,)),
            dma((3,)),
            dma((4, 2)),
            dma((4, 4)),
            dma((4,)),
            dma((4,)),
            dma((3,)),
            dma((4,)),
            dma((4, 4, 3)),
            dma((4, 4, 3)),
            dma((4, 4)),
            dma((4, 4)),
            dma((16,)),
            dma((16,)),
            dma((8,)),
            dma((8,)),
        ],
        compiler_params=pltpu.CompilerParams(
            collective_id=0, has_side_effects=True, vmem_limit_bytes=60 * 2**20
        ),
    )(
        clip_index.T, batch_order, clip_pool, tap_weights, out_weights, norm_gains,
        quant_weight.T, quant_bias, post_weight,
    )
    error, loss = pl.pallas_call(
        finish,
        out_shape=(
            jax.ShapeDtypeStruct((2, CLIPS, ROWS), F32),
            jax.ShapeDtypeStruct((1, 8), F32),
        ),
        in_specs=[vmem, vmem],
        out_specs=(vmem, vmem),
    )(error, loss)
    return error, loss.reshape(8)


def solution(mesh):
    torus = Mesh(
        mesh.devices.reshape(mesh.shape["section"], 4, 4, 2), ("section", "dp_0", "dp_1", "dp_2")
    )
    return jax.shard_map(
        on_device,
        mesh=torus,
        in_specs=(
            P(DP, None, None),
            P(None, DP),
            P(),
            P("section", None, None, None),
            P("section", None, None),
            P("section", None),
            P(),
            P(),
            P(),
        ),
        out_specs=(P("section", DP, None), P()),
        check_vma=False,
    )
```

```python
import functools

import jax
import jax.numpy as jnp
from jax import lax
from jax.experimental import pallas as pl
from jax.experimental.pallas import tpu as pltpu
from jax.sharding import Mesh
from jax.sharding import PartitionSpec as P


DP = ("dp_0", "dp_1", "dp_2")
MESH = pl.DeviceIdType.MESH
F32 = jnp.float32
BF16 = jnp.bfloat16
C = 512
BITS = 18
PAD = 32
CLIPS = 4
ROWS = 256
SPATIAL = 64
GROUP = CLIPS * ROWS
NORM_EPS = 1e-06
ROWS_TOTAL = 128.0 * 256.0
DIRECT = (0, 1)
LEFT = (2, 0, 3, 1)

SCHEDULE = (
    ("T", 2), ("V", 0), ("X", 0, 0), ("Y", 0), ("V", 1), ("T", 3), ("X", 0, 1), ("Y", 1), ("V", 2),
    ("X", 0, 2), ("Y", 2), ("V", 3), ("X", 0, 3), ("Y", 3), ("R", 0, 0), ("E", 0, 0), ("pool",),
    ("cs", 0, 0, 0), ("W", 0), ("X", 1, 0), ("R", 0, 1), ("cs", 0, 0, 1), ("W", 1), ("X", 1, 1), ("Z", 0),
    ("Z", 1), ("R", 0, 2), ("E", 0, 1), ("cs", 0, 1, 0), ("W", 2), ("X", 1, 2), ("cs", 0, 1, 1), ("X", 1, 3),
    ("W", 3), ("Z", 2), ("Z", 3), ("R", 0, 3), ("E", 0, 2), ("cs", 0, 2, 0), ("S", 0), ("cs", 0, 2, 1),
    ("R", 1, 0), ("E", 0, 3), ("cs", 0, 3, 0), ("X", 2, 0), ("X", 2, 1), ("cs", 0, 3, 1), ("R", 1, 1),
    ("X", 2, 2), ("X", 2, 3), ("prep",), ("L", 0), ("E", 1, 0), ("cs", 1, 0, 0), ("R", 1, 2), ("cs", 1, 0, 1),
    ("E", 1, 1), ("cs", 1, 1, 0), ("R", 1, 3), ("cs", 1, 1, 1), ("E", 1, 2), ("cs", 1, 2, 0), ("cs", 1, 2, 1),
    ("S", 1), ("E", 1, 3), ("cs", 1, 3, 0), ("cs", 1, 3, 1), ("R", 2, 0), ("quant",), ("s1send",),
    ("R", 2, 1), ("R", 2, 2), ("R", 2, 3), ("L", 1), ("E", 2, 0), ("E", 2, 1), ("E", 2, 2), ("ct", 2, 0),
    ("S", 2), ("ct", 2, 1), ("E", 2, 3), ("co", 2, 0), ("co", 2, 1), ("s1take",), ("s2send",), ("L", 2),
    ("cb", 3, 0), ("err", 0), ("cb", 3, 1), ("err", 1),
)


def dot(a, b):
    return jnp.dot(a, b, preferred_element_type=F32)


def dot_t(a, b):
    return lax.dot_general(a, b, (((1,), (1,)), ((), ())), preferred_element_type=F32)


def silu(u):
    return 0.5 * u * (1.0 + jnp.tanh(0.5 * u))


def rows_of(value, first, count):
    parts = value.reshape(CLIPS, -1, value.shape[-1])
    return parts[:, first : first + count].reshape(CLIPS * count, value.shape[-1])


def normalize(v, gain):
    wide = v.astype(F32)
    mean = jnp.mean(wide * wide, axis=-1, keepdims=True)
    return (wide * lax.rsqrt(mean + NORM_EPS) * gain).astype(BF16)


def taps(n, weight):
    p0 = dot(n, weight(0)).reshape(CLIPS, ROWS, C)
    p1 = dot(rows_of(n, 0, ROWS - SPATIAL), weight(1)).reshape(CLIPS, ROWS - SPATIAL, C)
    p2 = dot(rows_of(n, 0, ROWS - 2 * SPATIAL), weight(2)).reshape(CLIPS, ROWS - 2 * SPATIAL, C)
    mixed = jnp.concatenate(
        [
            p0[:, :SPATIAL],
            p0[:, SPATIAL : 2 * SPATIAL] + p1[:, :SPATIAL],
            p0[:, 2 * SPATIAL :] + p1[:, SPATIAL:] + p2,
        ],
        axis=1,
    )
    return mixed.reshape(GROUP, C)


def kernel(
    index_hbm, order_hbm, pool_hbm, taps_hbm, out_hbm, gains_hbm, qw_hbm, qb_hbm, pw_hbm,
    error_hbm, loss_hbm,
    pool, wts, gains, act, nrm, acc, index_ref, order_ref, qb, qw, pw, qwp, pwp, stat1, stat2, error_ref, loss_ref,
    lsem, osem, xs, xr, wr, gs, gr, rs, rr, ds, dr, s1s, s1r, s2s, s2r,
):
    x = lax.axis_index("section")
    y = lax.axis_index("dp_0")
    z = lax.axis_index("dp_1")
    c = lax.axis_index("dp_2")
    q = y * (1 - c) + z * c

    def xpeer(d):
        return (lax.rem(x + d, 4), y, z, c)

    def ring(d):
        return (x, lax.rem(y + d * (1 - c), 4), lax.rem(z + d * c, 4), c)

    def plane(dy, dz):
        return (x, lax.rem(y + dy, 4), lax.rem(z + dz, 4), c)

    def other(d, e):
        return (lax.rem(x + d, 4), y, z, lax.rem(c + e, 2))

    sibling = other(0, 1)
    near = [(d, 0) for d in (1, 2, 3)] + [(0, d) for d in (1, 2, 3)]
    planes = [(dy, dz) for dy in range(4) for dz in range(4) if dy or dz]
    others = [(d, e) for d in range(4) for e in range(2) if d or e]

    barrier = pltpu.get_barrier_semaphore()
    for dy, dz in near:
        pl.semaphore_signal(barrier, inc=1, device_id=plane(dy, dz), device_id_type=MESH)
    for d, e in others:
        pl.semaphore_signal(barrier, inc=1, device_id=other(d, e), device_id_type=MESH)
    loads = [
        (taps_hbm.at[0], wts.at[x, pl.ds(0, 3)]),
        (out_hbm.at[0], wts.at[x, 3]),
        (gains_hbm, gains.at[x]),
        (index_hbm, index_ref),
        (pool_hbm, pool),
        (order_hbm, order_ref),
        (qb_hbm, qb),
        (qw_hbm, qw),
        (pw_hbm, pw),
    ]
    loads = [pltpu.make_async_copy(a, b, lsem.at[i]) for i, (a, b) in enumerate(loads)]
    for load in loads:
        load.start()
    with jax.named_scope("barrier"):
        pl.semaphore_wait(barrier, len(near) + len(others))
    for load in loads[:3]:
        load.wait()

    def remote(ref, send, recv, device):
        return pltpu.make_async_remote_copy(
            ref, ref, send, recv, device_id=device, device_id_type=MESH
        )

    def arrived(ref, semaphore):
        pltpu.make_async_copy(ref, ref, semaphore).wait()

    def quarter(b, m, owner):
        return wts.at[b, m, pl.ds(pl.multiple_of(c * 256 + owner * 64, 64), 64)]

    def xcopy(b, m, d):
        return remote(quarter(b, m, q), xs, xr.at[b, m], xpeer(d))

    def relay(m):
        b = 3 - x
        return remote(quarter(b, m, q), xs, xr.at[b, m], xpeer(1 + 2 * lax.rem(x, 2)))

    def across(m):
        return remote(quarter(0, m, q), xs, xr.at[0, m], xpeer(2))

    def mate(m):
        return lax.rem(q + (1 if m % 2 == 0 else 3) + 2 * lax.rem(q, 2), 4)

    def second(m):
        return remote(quarter(1, m, mate(m)), xs, wr.at[m], xpeer(1))

    def gcopy(b, d):
        return remote(gains.at[b], gs.at[d - 1], gr.at[b], xpeer(d))

    def rcopy(b, m, d, owner):
        return remote(quarter(b, m, owner), rs, rr.at[b, m], ring(d))

    def dcopy(b, m, h):
        ref = wts.at[b, m, pl.ds(pl.multiple_of(h * 256, 256), 256)]
        return remote(ref, ds, dr.at[b, m], sibling)

    def foreign(f):
        return jnp.where(x <= f, f + 1, f)

    def own(m, d):
        xcopy(x, m, d).start()

    for m in range(4):

        @pl.when(x == 0)
        def _():
            own(m, 1)
            own(LEFT[m], 3)
            if m in DIRECT:
                across(m).start()

        @pl.when(x == 1)
        def _():
            own(m, 3)
            own(m, 1)

        @pl.when(x == 2)
        def _():
            own(m, 3)

        @pl.when(x == 3)
        def _():
            own(m, 1)

    @pl.when(x == 1)
    def _():
        for m in range(4):
            second(m).start()

    for d in (1, 3, 2):
        gcopy(x, d).start()

    def take(f, m):
        xcopy(foreign(f), m, 1).wait_recv()

    def pass_on(f, m):
        for d in (1, 3, 2):
            rcopy(foreign(f), m, d, q).start()

    def W(m):
        @pl.when(x == 2)
        def _():
            second(m).wait_recv()
            there = mate(m + 1)
            device = (x, there * (1 - c) + y * c, z * (1 - c) + there * c, c)
            for at in (q, mate(m)):
                remote(quarter(1, m, at), rs, rr.at[1, m], device).start()

    def V(m):
        @pl.when(x == 2)
        def _():
            take(1, m)
            relay(m).start()
            if m == 3:
                for k in range(4):
                    own(k, 1)

    def Y(m):
        @pl.when(x == 1)
        def _():
            take(1, m)
            relay(m).start()

    def T(m):
        @pl.when(x == 3)
        def _():
            take(0, m)
            relay(m).start()
            if m == 3:
                for k in range(4):
                    own(k, 3)

    def Z(m):
        @pl.when(x == 0)
        def _():
            take(2, m)
            relay(m).start()

    def X(f, m):
        if f == 0:
            if m in DIRECT:
                take(f, m)
            else:

                @pl.when(x < 3)
                def _():
                    take(f, m)

        elif f == 1:

            @pl.when((x == 0) | (x == 3))
            def _():
                take(f, m)
        else:

            @pl.when(x > 0)
            def _():
                take(f, m)

        if f == 1:

            @pl.when(x != 2)
            def _():
                pass_on(f, m)
        else:
            pass_on(f, m)

    def R(f, m):
        @pl.when(x > f)
        def _():
            gathered(f, m)

    def S(f):
        @pl.when(x <= f)
        def _():
            for m in range(4):
                gathered(f, m)

    def gathered(f, m):
        b = foreign(f)
        if f == 1:

            @pl.when(x == 2)
            def _():
                arrived(wts.at[b, m, pl.ds(0, 128)], rr.at[b, m])

            @pl.when(x != 2)
            def _():
                arrived(wts.at[b, m, pl.ds(0, 192)], rr.at[b, m])
        else:
            arrived(wts.at[b, m, pl.ds(0, 192)], rr.at[b, m])
        dcopy(b, m, c).start()

    def landed(f, m):
        dcopy(foreign(f), m, 1 - c).wait_recv()
        if m == 0:
            gcopy(foreign(f), 1).wait_recv()

    def E(f, m):
        @pl.when(x > f)
        def _():
            landed(f, m)

    def L(f):
        @pl.when(x <= f)
        def _():
            for m in range(4):
                landed(f, m)

    def group(g):
        return pl.ds(g * GROUP, GROUP)

    def gain(b):
        return gains[b].astype(F32)

    def source(i, k):
        return pool[index_ref[k, 2 * x + i]]

    def weight(b):
        return lambda m: wts[b, m]

    def cs(b, m, g):
        def part(n, skip):
            product = dot(rows_of(n, 0, ROWS - skip), wts[b, m]).reshape(CLIPS, ROWS - skip, C)
            for k in range(CLIPS):
                at = pl.ds(g * GROUP + k * ROWS + skip, ROWS - skip)
                acc[at, :] = acc[at, :] + product[k]

        if m == 0 or m == 3:
            if b == 0:
                v = jnp.concatenate([source(g, k) for k in range(CLIPS)], axis=0)
            else:
                v = act[group(g), :]
        if m == 0:
            n = normalize(v, gain(b))
            nrm[group(g), :] = n
            acc[group(g), :] = dot(n, wts[b, 0])
        elif m < 3:
            part(nrm[group(g), :], m * SPATIAL)
        else:
            a = silu(acc[group(g), :]).astype(BF16)
            act[group(g), :] = (v.astype(F32) + dot(a, wts[b, 3])).astype(BF16)

    def ct(b, g):
        n = normalize(act[group(g), :], gain(b))
        nrm[group(g), :] = silu(taps(n, weight(b))).astype(BF16)

    def co(b, g):
        wide = act[group(g), :].astype(F32)
        act[group(g), :] = (wide + dot(nrm[group(g), :], wts[b, 3])).astype(BF16)

    def cb(b, g):
        v = act[group(g), :]
        n = normalize(v, gain(b))
        a = silu(taps(n, weight(b))).astype(BF16)
        act[group(g), :] = (v.astype(F32) + dot(a, wts[b, 3])).astype(BF16)

    lane = lax.broadcasted_iota(jnp.int32, (8, 128), 1)
    row = lax.broadcasted_iota(jnp.int32, (8, 128), 0)

    def quantize(g):
        t = 4.0 * (dot_t(qwp[...], act[group(g), :]) + bias())
        codes = jnp.tanh(0.5 * t)
        back = lax.dot_general(
            codes.astype(BF16), pwp[...], (((0,), (0,)), ((), ())), preferred_element_type=F32
        )
        act[group(g), :] = back.astype(BF16)
        size = jnp.abs(t)
        e = jnp.exp(-size)
        entropy = jnp.log(1.0 + e) + size * e / (1.0 + e)
        bit = jnp.sum(0.5 * (1.0 + codes), axis=1, keepdims=True)
        ent = jnp.sum(entropy, axis=1, keepdims=True)
        at = lax.broadcasted_iota(jnp.int32, (PAD, 128), 0)
        col = lax.broadcasted_iota(jnp.int32, (PAD, 128), 1)
        bit = jnp.sum(jnp.where((at == col) & (col < BITS), bit, 0.0), axis=0, keepdims=True)
        ent = jnp.sum(jnp.where((at < BITS) & (col == BITS), ent, 0.0), axis=0, keepdims=True)
        return jnp.where(row == 2 * x + g, bit + ent, 0.0)

    def bias():
        at = lax.broadcasted_iota(jnp.int32, (PAD, 1), 0)
        value = jnp.zeros((PAD, 1), F32)
        for k in range(BITS):
            value = jnp.where(at == k, qb[k], value)
        return value

    def s1copy(dy, dz, sy, sz):
        ref = stat1.at[sy * 4 + sz]
        return remote(ref, s1s, s1r, plane(dy, dz))

    def s2copy(d, e, sx, sc):
        ref = stat2.at[sx * 2 + sc]
        return remote(ref, s2s, s2r, other(d, e))

    stored = [
        pltpu.make_async_copy(error_ref.at[g], error_hbm.at[g], osem.at[g]) for g in range(2)
    ] + [pltpu.make_async_copy(loss_ref, loss_hbm, osem.at[2])]

    def errors(g):
        for k in range(CLIPS):
            at = pl.ds(g * GROUP + k * ROWS, ROWS)
            differ = act[at, :].astype(F32) - source(g, k).astype(F32)
            square = differ * differ
            part = square[:, :128] + square[:, 128:256] + square[:, 256:384] + square[:, 384:]
            total = jnp.sum(part.T, axis=0, keepdims=True)
            error_ref[g, k : k + 1, :] = total * (1.0 / C)
        stored[g].start()

    def pool_ready():
        loads[3].wait()
        loads[4].wait()

    def quantizers():
        for load in loads[5:]:
            load.wait()
        qwp[...] = jnp.zeros_like(qwp)
        pwp[...] = jnp.zeros_like(pwp)
        qwp[0:BITS, :] = qw[...]
        pwp[0:BITS, :] = pw[...]

    def quantize_both():
        stat1[y * 4 + z] = quantize(0) + quantize(1)

    def s1send():
        for dy, dz in planes:
            s1copy(dy, dz, y, z).start()

    def s1take():
        arrived(stat1.at[pl.ds(0, 15)], s1r)
        total = stat1[0]
        for k in range(1, 16):
            total = total + stat1[k]
        stat2[x * 2 + c] = total

    def s2send():
        for d, e in others:
            s2copy(d, e, x, c).start()

    steps = {
        "X": X, "T": T, "W": W, "S": S, "Y": Y, "V": V, "Z": Z, "R": R, "E": E, "L": L, "cs": cs, "ct": ct, "co": co, "cb": cb, "err": errors, "pool": pool_ready,
        "prep": quantizers, "quant": quantize_both, "s1send": s1send, "s1take": s1take, "s2send": s2send,
    }
    for name, *numbers in SCHEDULE:
        with jax.named_scope("_".join(map(str, [name, *numbers]))):
            steps[name](*numbers)

    with jax.named_scope("s2take"):
        arrived(stat2.at[pl.ds(0, 7)], s2r)
    with jax.named_scope("loss"):
        total = stat2[0]
        for k in range(1, 8):
            total = total + stat2[k]
        mean = total / ROWS_TOTAL
        averaged = jnp.zeros((8, 128), F32)
        running = None
        for t in range(8):
            chosen = row == order_ref[t]
            marginal = jnp.sum(jnp.where(chosen, mean, 0.0), axis=0, keepdims=True)
            running = marginal if t == 0 else 0.5 * running + 0.5 * marginal
            averaged = jnp.where(chosen, running, averaged)
        smoothed = 0.05 + 0.9 * averaged
        smoothed = jnp.where(lane < BITS, smoothed, 0.5)
        terms = smoothed * jnp.log(smoothed) + (1.0 - smoothed) * jnp.log(1.0 - smoothed)
        terms = jnp.where(lane < BITS, terms, jnp.where(lane == BITS, mean, 0.0))
        loss = jnp.sum(terms, axis=1, keepdims=True)
        loss_ref[...] = jnp.sum(jnp.where(row == lane, loss, 0.0), axis=0, keepdims=True)

    stored[2].start()

    with jax.named_scope("sent"):
        for d in (1, 3, 2):
            gcopy(x, d).wait_send()
        arrived(wts.at[0, 0], xs)
        for count, mine in ((384, x == 0), (512, x == 1), (256, x == 2), (128, x == 3)):

            @pl.when(mine)
            def _(count=count):
                arrived(wts.at[0, 0, pl.ds(0, count)], xs)

        for k in range(8):
            arrived(wts.at[0, 0, pl.ds(0, 256)], rs)

        @pl.when(x != 2)
        def _():
            arrived(wts.at[0, 0, pl.ds(0, 256)], rs)

        for k in range(6):
            arrived(wts.at[0, 0], ds)
        arrived(stat1.at[pl.ds(0, 15)], s1s)
        arrived(stat2.at[pl.ds(0, 7)], s2s)
    with jax.named_scope("stored"):
        for copy in stored:
            copy.wait()


def finish(error_in, loss_in, error_out, loss_out):
    error_out[...] = error_in[...]
    loss_out[...] = loss_in[:, 0:8]


def on_device(
    clip_pool, clip_index, batch_order, tap_weights, out_weights, norm_gains,
    quant_weight, quant_bias, post_weight,
):
    any_space = pl.BlockSpec(memory_space=pl.ANY)
    vmem = pl.BlockSpec(memory_space=pltpu.VMEM)
    dma = pltpu.SemaphoreType.DMA
    error, loss = pl.pallas_call(
        kernel,
        out_shape=(
            jax.ShapeDtypeStruct((2, CLIPS, ROWS), F32),
            jax.ShapeDtypeStruct((1, 128), F32),
        ),
        in_specs=[any_space] * 9,
        out_specs=(any_space, any_space),
        scratch_shapes=[
            pltpu.VMEM((32, ROWS, C), BF16),
            pltpu.VMEM((4, 4, C, C), BF16),
            pltpu.VMEM((4, 1, C), BF16),
            pltpu.VMEM((2 * GROUP, C), BF16),
            pltpu.VMEM((2 * GROUP, C), BF16),
            pltpu.VMEM((2 * GROUP, C), F32),
            pltpu.SMEM((CLIPS, 8), jnp.int32),
            pltpu.SMEM((8,), jnp.int32),
            pltpu.SMEM((BITS,), F32),
            pltpu.VMEM((BITS, C), BF16),
            pltpu.VMEM((BITS, C), BF16),
            pltpu.VMEM((PAD, C), BF16),
            pltpu.VMEM((PAD, C), BF16),
            pltpu.VMEM((16, 8, 128), F32),
            pltpu.VMEM((8, 8, 128), F32),
            pltpu.VMEM((2, CLIPS, ROWS), F32),
            pltpu.VMEM((1, 128), F32),
            dma((9,)),
            dma((3,)),
            dma,
            dma((4, 4)),
            dma((4,)),
            dma((3,)),
            dma((4,)),
            dma,
            dma((4, 4)),
            dma,
            dma((4, 4)),
            dma,
            dma,
            dma,
            dma,
        ],
        compiler_params=pltpu.CompilerParams(
            collective_id=0, has_side_effects=True, vmem_limit_bytes=60 * 2**20
        ),
    )(
        clip_index.T, batch_order, clip_pool, tap_weights, out_weights, norm_gains,
        quant_weight.T, quant_bias, post_weight,
    )
    error, loss = pl.pallas_call(
        finish,
        out_shape=(
            jax.ShapeDtypeStruct((2, CLIPS, ROWS), F32),
            jax.ShapeDtypeStruct((1, 8), F32),
        ),
        in_specs=[vmem, vmem],
        out_specs=(vmem, vmem),
    )(error, loss)
    return error, loss.reshape(8)


def solution(mesh):
    torus = Mesh(
        mesh.devices.reshape(mesh.shape["section"], 4, 4, 2), ("section", "dp_0", "dp_1", "dp_2")
    )
    return jax.shard_map(
        on_device,
        mesh=torus,
        in_specs=(
            P(DP, None, None),
            P(None, DP),
            P(),
            P("section", None, None, None),
            P("section", None, None),
            P("section", None),
            P(),
            P(),
            P(),
        ),
        out_specs=(P("section", DP, None), P()),
        check_vma=False,
    )
```
